32 devices in a mesh: band: 8 (over y, x, core), lev: 4 (over z).
Axes of the slice: x: 2, y: 2, z: 4, core: 2. Of those that a mesh axis runs over, the one named last changes fastest.
Arguments:
- pattern: float32 [1024, 128], P('band'), may hold values from -3 to 3
- taper: float32 [136], P('lev'), may hold values from 0.1 to 1
- thickness: float32 [136], P('lev'), may hold values from 0.2 to 2
- block_source: int32 [1024], P('band'), may hold values from 0 to 1023, as said below
- tendencies: bfloat16 [4, 136, 131072], P(None, 'lev', 'band'), may hold values from -6 to 6
Outputs:
- perturbed: bfloat16 [4, 136, 131072], P(None, 'lev', 'band')
- integrals: float32 [2, 131072], P(None, 'band')
The draws below stay inside these ranges and needn't reach their ends.
Inputs may be any that keep to these rules, and one draw needn't show every extreme that they name: block_source is a permutation of 0 to 1023; the 128 physics blocks of each band index take exactly 128 // 8 grid blocks from the 128 grid blocks of each band index.
All inputs are finite; a program needn't handle non-finite values.
Results may differ from the reference program's by a relative error of at most 0.001.
Values sent between devices are 32-bit elements; how exact they have to be, the bound alone decides.
A program may use at most 64 MiB of HBM per device.

```python
import math
import jax
import jax.numpy as jnp
from jax import lax

BLOCK = 128
LEV = 136
BLK_DEV = 128
NBLK = 1024
COLUMNS = 131072


def draw_block_source(key, part):
    bands = NBLK // BLK_DEV
    share = BLK_DEV // bands
    first_key, second_key = jax.random.split(jax.random.fold_in(key, 11))
    labels = jnp.repeat(jnp.arange(bands, dtype=jnp.int32), share)
    owner_keys = jax.random.split(first_key, bands)
    owners = jax.vmap(lambda k: jax.random.permutation(k, labels))(owner_keys).reshape(-1)
    grouped = jnp.argsort(owners, stable=True).astype(jnp.int32).reshape(bands, BLK_DEV)
    row_keys = jax.random.split(second_key, bands)
    shuffled = jax.vmap(lambda k, row: jax.random.permutation(k, row))(row_keys, grouped)
    return shuffled.reshape(-1).astype(jnp.int32)


def steps_of(stream_key, extent, pieces, low, top_value):
    gain, own = 1.0, jax.random.fold_in(stream_key, 6)
    for position, blocks in pieces:
        draws = jnp.exp(jax.random.uniform(jax.random.fold_in(own, position), (blocks,), jnp.float32, low / len(pieces), top_value / len(pieces)))
        gain = gain * jnp.repeat(draws, extent[position] // blocks).reshape([-1 if axis == position else 1 for axis in range(len(extent))])
    return gain


def gaussian(stream_key, extent, deviation, most, shards=(), kind=jnp.bfloat16):
    result = jax.random.normal(stream_key, extent, jnp.float32) * deviation
    if len(shards) > 0:
        result = steps_of(stream_key, extent, shards, -0.22, 0.18) * result
    return jnp.clip(result, min=-most, max=most).astype(kind)


def setup_inputs(seed: int = 0) -> dict:
    keys = jax.random.split(jax.random.key(seed), 6)
    return {
        "pattern": gaussian(keys[0], (NBLK, BLOCK), 0.6, 3.0, ((0, 8),), jnp.float32),
        "taper": jnp.clip(0.1 + 0.9 * jax.random.uniform(keys[1], (LEV,), jnp.float32) ** steps_of(keys[1], (LEV,), ((0, 4),), -0.2, 0.2), 0.1, 1.0),
        "thickness": jnp.clip(jnp.exp(math.log(2.0) - 2.3025851 * jax.random.uniform(keys[2], (LEV,), jnp.float32) ** steps_of(keys[2], (LEV,), ((0, 4),), -0.2, 0.2)), 0.2, 2.0),
        "block_source": draw_block_source(jax.random.fold_in(keys[5], 71), 0),
        "tendencies": gaussian(keys[4], (4, LEV, COLUMNS), 1.0, 6.0, ((1, 4), (2, 8))),
    }


def reference(pattern, taper, thickness, block_source, tendencies):
    clipped = jnp.tanh(pattern)
    local = jnp.take(clipped, block_source, axis=0).reshape(-1)
    pert = taper[:, None] * local[None, :]

    def scale_field(field):
        return (field.astype(jnp.float32) * (1.0 + pert)).astype(jnp.bfloat16)
    perturbed = lax.map(scale_field, tendencies)

    def column_sum(field):
        return lax.optimization_barrier(jnp.sum(thickness[:, None] * field.astype(jnp.float32) * pert, axis=0))
    norm_value = jnp.sqrt(jnp.sum(thickness * thickness))
    integrals = lax.map(column_sum, tendencies[2:4]) / norm_value
    return (perturbed, integrals)
```

```python
import functools
import jax
import jax.numpy as jnp
from jax import lax
from jax.experimental import pallas as pl
from jax.experimental.pallas import tpu as pltpu
from jax.sharding import PartitionSpec as P

MESH = pl.DeviceIdType.MESH


def exchange(n_band, n_lev, pattern, source_hbm, taper_hbm, thickness_hbm, tend, made, sums,
             held, spread, whole, acc, part, inbox, totals, partial, outgoing, source, taper, thickness,
             small_sem, own_sem, load_sem, ready, mate_ready, lev_ready, out_sem, in_sem, pass_sem,
             part_send, part_recv, partial_send, total_send, total_recv):
    band, lev = lax.axis_index("band"), lax.axis_index("lev")
    levels, rows, lanes = tend.shape
    blocks = pattern.shape[0]
    fields = rows // blocks
    pieces, half = totals.shape[0], n_lev // 2
    share, piece = blocks // pieces, rows // pieces
    pairs = n_band // 2
    per = pieces // 2
    side = lev // half
    near, far = half - 1 + side, half - side
    pair, core = band // 2, band % 2
    hub, keeper = core == 0, 2 * pair + 1
    owner = (core == 1) & (lev == near)

    def signal(sem, **where):
        pl.semaphore_signal(sem, inc=1, device_id=where, device_id_type=MESH)

    def block_rows(who):
        return pl.ds(pl.multiple_of(who * blocks, blocks), blocks)

    barrier = pltpu.get_barrier_semaphore()
    for t in range(half - 1, half + 1):
        pl.when(lev < t)(lambda t=t: signal(barrier, band=keeper, lev=t))
    for t in range(half, n_lev):
        @pl.when(owner & (lev < t))
        def _(t=t):
            signal(barrier, band=2 * pair, lev=t)
            if t > half:
                signal(barrier, band=keeper, lev=t)
    pl.when(hub)(lambda: signal(barrier, band=keeper))
    for t in range(1, pairs):
        @pl.when(pair < t)
        def _(t=t):
            signal(barrier, band=2 * t)
            pl.when(hub)(lambda: signal(barrier, band=2 * t + 1))
    from_band = jnp.where(hub, 2 * pair, pair + 1)
    from_lev = jnp.where(lev > half, 2, jnp.where(hub, lev // half, jnp.where(lev < half - 1, 0, 2 * lev)))
    expected = from_band + from_lev

    own = pltpu.make_async_copy(pattern, whole.at[block_rows(band)], own_sem)
    own.start()
    small = [pltpu.make_async_copy(a, b, small_sem.at[i]) for i, (a, b) in enumerate(
        ((thickness_hbm, thickness), (taper_hbm, taper), (source_hbm, source)))]
    for copy in small:
        copy.start()

    def chunk_of(step):
        return (1 - side if step % 2 == 0 else side) * per + step // 2

    def load(step):
        span = pl.ds(pl.multiple_of(chunk_of(step) * piece, piece), piece)
        return pltpu.make_async_copy(tend.at[:, span, :], held.at[:, span, :], load_sem.at[step])

    for step in range(pieces):
        load(step).start()

    def direct(t):
        mine = whole.at[block_rows(band)]
        return pltpu.make_async_remote_copy(mine, mine, out_sem.at[t], in_sem.at[band],
                                            device_id={"band": 2 * t}, device_id_type=MESH)

    def relay(origin):
        block = whole.at[block_rows(origin)]
        return pltpu.make_async_remote_copy(block, block, pass_sem.at[origin], in_sem.at[origin],
                                            device_id={"band": keeper}, device_id_type=MESH)

    def came(origin):
        block = whole.at[block_rows(origin)]
        pltpu.make_async_remote_copy(block, block, pass_sem.at[origin], in_sem.at[origin],
                                     device_id={"band": band + 1 - 2 * core}, device_id_type=MESH).wait_recv()

    def give(step):
        where = {"band": keeper, "lev": far if step % 2 == 0 else near}
        return pltpu.make_async_remote_copy(part.at[step], inbox.at[core, lev, step // 2], part_send.at[step],
                                            part_recv.at[core, lev, step // 2],
                                            device_id=where, device_id_type=MESH)

    def got(c, e, q):
        pltpu.make_async_remote_copy(part.at[q], inbox.at[c, e, q], part_send.at[q], part_recv.at[c, e, q],
                                     device_id={"lev": far}, device_id_type=MESH).wait_recv()

    def publish_first(c, q):
        return pltpu.make_async_remote_copy(partial.at[c, q], totals.at[side * per + q], partial_send.at[c, q],
                                            total_recv.at[side * per + q],
                                            device_id={"band": 2 * pair + c, "lev": 0}, device_id_type=MESH)

    def publish(c, t, q):
        return pltpu.make_async_remote_copy(outgoing.at[c, q], totals.at[side * per + q], total_send.at[c, t, q],
                                            total_recv.at[side * per + q],
                                            device_id={"band": 2 * pair + c, "lev": t}, device_id_type=MESH)

    def elsewhere(c, t):
        return True if c == 0 else lev != t

    pl.when(expected > 0)(lambda: pl.semaphore_wait(barrier, expected))
    for t in range(half):
        @pl.when(owner & (lev > t))
        def _(t=t):
            signal(lev_ready.at[side], band=2 * pair, lev=t)
            signal(lev_ready.at[side], band=keeper, lev=t)
    pl.when(core == 1)(lambda: signal(mate_ready, band=2 * pair))
    for t in range(pairs - 1):
        @pl.when(hub & (pair > t))
        def _(t=t):
            signal(ready.at[pair], band=2 * t)
            signal(ready.at[pair], band=2 * t + 1)
    own.wait()
    for t in range(pairs):
        pl.when((pair > t) | ((core == 1) & (pair == t)))(lambda t=t: direct(t).start())

    for copy in small:
        copy.wait()
    squares = thickness[0] * thickness[0]
    for l in range(1, levels):
        squares += thickness[l] * thickness[l]
    pl.when(hub)(lambda: pl.semaphore_wait(mate_ready, 1))
    for step in range(pieces):
        load(step).wait()
        first = pl.multiple_of(chunk_of(step) * piece, piece)
        for r in range(0, piece, 64):
            def add(l, total):
                weight = thickness[l] * taper[l]
                return total + weight * held[l, pl.ds(first + r, 64), :].astype(jnp.float32)
            acc[pl.ds(r, 64), :] = lax.fori_loop(0, levels, add, jnp.zeros((64, lanes), jnp.float32), unroll=34)
        for k in range(2):
            part[step, k * share:(k + 1) * share, :] = acc[pl.ds(fields - 2 + k, share, stride=fields), :]
        part[step, 2 * share:, :] = jnp.full((1, lanes), squares, jnp.float32)
        if step == 0:
            pl.when(lev < half)(lambda: pl.semaphore_wait(lev_ready.at[1], 1))
            give(step).start()
        elif step == 1:
            pl.when(lev < half - 1)(lambda: pl.semaphore_wait(lev_ready.at[0], 1))
        if step % 2 == 0:
            if step:
                give(step).start()
        else:
            pl.when(jnp.logical_not(owner))(lambda step=step: give(step).start())
    for t in range(1, pairs):
        @pl.when(pair < t)
        def _(t=t):
            pl.semaphore_wait(ready.at[t], 1)
            direct(t).start()

    @pl.when(owner)
    def _():
        for q in range(per):
            inbox[1, lev, q] = part[2 * q + 1]
        for c in (1, 0):
            for q in range(per):
                for e in range(1, n_lev):
                    pl.when(elsewhere(c, e))(lambda c=c, e=e, q=q: got(c, e, q))
                total = inbox[c, 1, q]
                for e in range(2, n_lev):
                    total = total + inbox[c, e, q]
                partial[c, q] = total
                publish_first(c, q).start()
        for c in (1, 0):
            for q in range(per):
                got(c, 0, q)
                total = inbox[c, 0, q] + partial[c, q]
                outgoing[c, q] = total
                if c == 1:
                    totals[side * per + q] = total
                for t in reversed(range(1, n_lev)):
                    pl.when(elsewhere(c, t))(lambda c=c, t=t, q=q: publish(c, t, q).start())

    @pl.when(hub)
    def _():
        relay(band).start()
        for c in range(2):
            for t in range(pairs):
                @pl.when(pair != t)
                def _(t=t, c=c):
                    came(2 * t + c)
                    relay(2 * t + c).start()
        came(band + 1)

    @pl.when(core == 1)
    def _():
        came(band - 1)
        for c in range(2):
            for t in range(pairs):
                pl.when(pair != t)(lambda t=t, c=c: came(2 * t + c))

    def pick(j, _):
        row = whole[pl.ds(source[j], 1), :]
        spread[pl.ds(pl.multiple_of(j * fields, fields), fields), :] = jnp.broadcast_to(row, (fields, lanes))
        return 0

    lax.fori_loop(0, blocks, pick, 0, unroll=32)

    def scale(i, _):
        span = pl.ds(pl.multiple_of(i * 64, 64), 64)
        local = jnp.tanh(spread[span, :])
        spread[span, :] = local

        def level(l, _):
            made[l, span, :] = (held[l, span, :].astype(jnp.float32) * (1.0 + taper[l] * local)).astype(made.dtype)
            return 0

        return lax.fori_loop(0, levels, level, 0, unroll=34)

    lax.fori_loop(0, rows // 64, scale, 0)

    for c in range(pieces):
        @pl.when(jnp.logical_not(owner & (side == c // per)))
        def _(c=c):
            pltpu.make_async_remote_copy(totals.at[c], totals.at[c], total_send.at[0, 0, 0], total_recv.at[c],
                                         device_id={"lev": far}, device_id_type=MESH).wait_recv()

        @pl.when(lev == 0)
        def _(c=c):
            totals[c] = part[2 * (c % per) + 1 - c // per] + totals[c]

        scaled = 1.0 / jnp.sqrt(totals[c, 2 * share:2 * share + 1, :])
        local = spread[pl.ds(c * share * fields, share, stride=fields), :] * scaled
        for k in range(2):
            sums[pl.ds(c * 2 * share + k, share, stride=2), :] = totals[c, k * share:(k + 1) * share, :] * local

    for step in range(pieces):
        if step % 2 == 0:
            give(step).wait_send()
        else:
            pl.when(jnp.logical_not(owner))(lambda step=step: give(step).wait_send())

    @pl.when(owner)
    def _():
        for c in range(2):
            for q in range(per):
                publish_first(c, q).wait_send()
                for t in range(1, n_lev):
                    pl.when(elsewhere(c, t))(lambda c=c, t=t, q=q: publish(c, t, q).wait_send())

    for t in range(pairs):
        pl.when((core == 1) | (pair != t))(lambda t=t: direct(t).wait_send())

    @pl.when(hub)
    def _():
        relay(band).wait_send()
        for c in range(2):
            for t in range(pairs):
                pl.when(pair != t)(lambda t=t, c=c: relay(2 * t + c).wait_send())


def write(made, sums, out, column, out_sem, sum_sem):
    copies = (pltpu.make_async_copy(made, out, out_sem), pltpu.make_async_copy(sums, column, sum_sem))
    for copy in copies:
        copy.start()
    for copy in copies:
        copy.wait()


def body(n_band, n_lev, pattern, taper, thickness, block_source, tendencies):
    assert n_lev == 4 and n_band % 2 == 0
    fields, levels, columns = tendencies.shape
    blocks, lanes = pattern.shape
    rows = blocks * fields
    pieces = 4
    share, piece, pairs = blocks // pieces, rows // pieces, n_band // 2
    per = pieces // 2
    tend = tendencies.transpose(1, 0, 2).reshape(levels, fields, blocks, lanes)
    tend = tend.transpose(0, 2, 1, 3).reshape(levels, rows, lanes)
    hbm = pl.BlockSpec(memory_space=pltpu.HBM)
    vector = pl.BlockSpec(memory_space=pltpu.VMEM)
    f32, dma, flag = jnp.float32, pltpu.SemaphoreType.DMA, pltpu.SemaphoreType.REGULAR
    made, sums = pl.pallas_call(
        functools.partial(exchange, n_band, n_lev),
        name="exchange",
        out_shape=(pltpu.VMEM(tend.shape, tend.dtype), pltpu.VMEM((2 * blocks, lanes), f32)),
        in_specs=[hbm] * 5,
        out_specs=(vector, vector),
        scratch_shapes=[
            pltpu.VMEM(tend.shape, tend.dtype),
            pltpu.VMEM((rows, lanes), f32),
            pltpu.VMEM((n_band * blocks, lanes), f32),
            pltpu.VMEM((piece, lanes), f32),
            pltpu.VMEM((pieces, 2 * share + 1, lanes), f32),
            pltpu.VMEM((2, n_lev, per, 2 * share + 1, lanes), f32),
            pltpu.VMEM((pieces, 2 * share + 1, lanes), f32),
            pltpu.VMEM((2, per, 2 * share + 1, lanes), f32),
            pltpu.VMEM((2, per, 2 * share + 1, lanes), f32),
            pltpu.SMEM(block_source.shape, jnp.int32), pltpu.SMEM(taper.shape, f32), pltpu.SMEM(thickness.shape, f32),
            dma((3,)), dma, dma((pieces,)),
            flag((pairs,)), flag, flag((2,)),
            dma((pairs,)), dma((n_band,)), dma((n_band,)),
            dma((pieces,)), dma((2, n_lev, per)), dma((2, per)), dma((2, n_lev, per)), dma((pieces,)),
        ],
        compiler_params=pltpu.CompilerParams(collective_id=0, has_side_effects=True, vmem_limit_bytes=24 << 20),
    )(*(pltpu.with_memory_space_constraint(x, pltpu.MemorySpace.HBM)
        for x in (pattern, block_source, taper, thickness, tend)))
    in_vmem = lambda x: pltpu.with_memory_space_constraint(x, pltpu.MemorySpace.VMEM)
    out, column = pl.pallas_call(
        write,
        name="write",
        out_shape=(jax.ShapeDtypeStruct(tend.shape, tend.dtype), jax.ShapeDtypeStruct((2 * blocks, lanes), f32)),
        in_specs=[vector, vector],
        out_specs=(hbm, hbm),
        scratch_shapes=[dma, dma],
        compiler_params=pltpu.CompilerParams(vmem_limit_bytes=1 << 20),
    )(in_vmem(made), in_vmem(sums))
    out = out.reshape(levels, blocks, fields, lanes).transpose(2, 0, 1, 3).reshape(fields, levels, columns)
    return out, column.reshape(blocks, 2, lanes).transpose(1, 0, 2).reshape(2, columns)


def solution(mesh):
    in_specs = (P("band", None), P("lev"), P("lev"), P("band"), P(None, "lev", "band"))
    out_specs = (P(None, "lev", "band"), P(None, "band"))
    run = functools.partial(body, mesh.shape["band"], mesh.shape["lev"])
    return jax.shard_map(run, mesh=mesh, in_specs=in_specs, out_specs=out_specs, check_vma=False)
```

```python
import functools
import jax
import jax.numpy as jnp
from jax import lax
from jax.experimental import pallas as pl
from jax.experimental.pallas import tpu as pltpu
from jax.sharding import PartitionSpec as P

MESH = pl.DeviceIdType.MESH


def exchange(n_band, n_lev, pattern, source_hbm, taper_hbm, thickness_hbm, tend, made, sums,
             held, spread, whole, acc, part, inbox, totals, partial, outgoing, source, taper, thickness,
             small_sem, own_sem, load_sem, ready, mate_ready, lev_ready, in_sem, part_recv, total_recv):
    band, lev = lax.axis_index("band"), lax.axis_index("lev")
    levels, rows, lanes = tend.shape
    blocks = pattern.shape[0]
    fields = rows // blocks
    pieces, half = totals.shape[0], n_lev // 2
    share, piece = blocks // pieces, rows // pieces
    pairs = n_band // 2
    per = pieces // 2
    side = lev // half
    near, far = half - 1 + side, half - side
    pair, core = band // 2, band % 2
    hub, keeper = core == 0, 2 * pair + 1
    owner = (core == 1) & (lev == near)
    out_sem, pass_sem, part_send, publish_send = own_sem, small_sem.at[0], small_sem.at[1], load_sem

    def signal(sem, **where):
        pl.semaphore_signal(sem, inc=1, device_id=where, device_id_type=MESH)

    def block_rows(who):
        return pl.ds(pl.multiple_of(who * blocks, blocks), blocks)

    barrier = pltpu.get_barrier_semaphore()
    for t in range(half - 1, half + 1):
        pl.when(lev < t)(lambda t=t: signal(barrier, band=keeper, lev=t))
    for t in range(half, n_lev):
        @pl.when(owner & (lev < t))
        def _(t=t):
            signal(barrier, band=2 * pair, lev=t)
            if t > half:
                signal(barrier, band=keeper, lev=t)
    pl.when(hub)(lambda: signal(barrier, band=keeper))
    for t in range(1, pairs):
        @pl.when(pair < t)
        def _(t=t):
            signal(barrier, band=2 * t)
            pl.when(hub)(lambda: signal(barrier, band=2 * t + 1))
    from_band = jnp.where(hub, 2 * pair, pair + 1)
    from_lev = jnp.where(lev > half, 2, jnp.where(hub, lev // half, jnp.where(lev < half - 1, 0, 2 * lev)))
    expected = from_band + from_lev

    own = pltpu.make_async_copy(pattern, whole.at[block_rows(band)], own_sem)
    own.start()
    small = [pltpu.make_async_copy(a, b, small_sem.at[i]) for i, (a, b) in enumerate(
        ((thickness_hbm, thickness), (taper_hbm, taper), (source_hbm, source)))]
    for copy in small:
        copy.start()

    def chunk_of(step):
        return (1 - side if step % 2 == 0 else side) * per + step // 2

    def load(step):
        span = pl.ds(pl.multiple_of(chunk_of(step) * piece, piece), piece)
        return pltpu.make_async_copy(tend.at[:, span, :], held.at[:, span, :], load_sem.at[step])

    for step in range(pieces):
        load(step).start()

    def direct(t):
        mine = whole.at[block_rows(band)]
        return pltpu.make_async_remote_copy(mine, mine, out_sem, in_sem.at[band],
                                            device_id={"band": 2 * t}, device_id_type=MESH)

    def relay(origin):
        block = whole.at[block_rows(origin)]
        return pltpu.make_async_remote_copy(block, block, pass_sem, in_sem.at[0],
                                            device_id={"band": keeper}, device_id_type=MESH)

    def remote(ref, send, receive):
        return pltpu.make_async_remote_copy(ref, ref, send, receive,
                                            device_id={"lev": far}, device_id_type=MESH)

    def came(origin):
        remote(whole.at[block_rows(origin)], pass_sem, in_sem.at[origin]).wait_recv()

    def give(step):
        where = {"band": keeper, "lev": far if step % 2 == 0 else near}
        return pltpu.make_async_remote_copy(part.at[step], inbox.at[core, step // 2, lev], part_send,
                                            part_recv.at[core, jnp.where(lev == 0, per, step // 2)],
                                            device_id=where, device_id_type=MESH)

    def publish_first(c, q):
        return pltpu.make_async_remote_copy(partial.at[c, q], totals.at[side * per + q], publish_send.at[c], total_recv,
                                            device_id={"band": 2 * pair + c, "lev": 0}, device_id_type=MESH)

    def publish(c, t, q):
        return pltpu.make_async_remote_copy(outgoing.at[c, q], totals.at[side * per + q], publish_send.at[c], total_recv,
                                            device_id={"band": 2 * pair + c, "lev": t}, device_id_type=MESH)

    def elsewhere(c, t):
        return True if c == 0 else lev != t

    pl.when(expected > 0)(lambda: pl.semaphore_wait(barrier, expected))
    for t in range(half):
        @pl.when(owner & (lev > t))
        def _(t=t):
            signal(lev_ready, band=2 * pair, lev=t)
            signal(lev_ready, band=keeper, lev=t)
    pl.when(core == 1)(lambda: signal(mate_ready, band=2 * pair))
    for t in range(pairs - 1):
        @pl.when(hub & (pair > t))
        def _(t=t):
            signal(ready, band=2 * t)
            signal(ready, band=2 * t + 1)
    own.wait()
    for t in range(pairs):
        pl.when((pair > t) | ((core == 1) & (pair == t)))(lambda t=t: direct(t).start())

    for copy in small:
        copy.wait()
    squares = thickness[0] * thickness[0]
    for l in range(1, levels):
        squares += thickness[l] * thickness[l]
    pl.when(hub)(lambda: pl.semaphore_wait(mate_ready, 1))
    for step in range(pieces):
        load(step).wait()
        first = pl.multiple_of(chunk_of(step) * piece, piece)
        for r in range(0, piece, 64):
            def add(l, total):
                weight = thickness[l] * taper[l]
                return total + weight * held[l, pl.ds(first + r, 64), :].astype(jnp.float32)
            acc[pl.ds(r, 64), :] = lax.fori_loop(0, levels, add, jnp.zeros((64, lanes), jnp.float32), unroll=34)
        for k in range(2):
            part[step, k * share:(k + 1) * share, :] = acc[pl.ds(fields - 2 + k, share, stride=fields), :]
        part[step, 2 * share:, :] = jnp.full((1, lanes), squares, jnp.float32)
        if step == 0:
            pl.when(lev < half)(lambda: pl.semaphore_wait(lev_ready, jnp.where(lev < half - 1, 2, 1)))
        if step % 2 == 0:
            give(step).start()
        else:
            pl.when(jnp.logical_not(owner))(lambda step=step: give(step).start())
    pl.when(pair < pairs - 1)(lambda: pl.semaphore_wait(ready, pairs - 1 - pair))
    for t in range(1, pairs):
        pl.when(pair < t)(lambda t=t: direct(t).start())

    @pl.when(owner)
    def _():
        for q in range(per):
            inbox[1, q, lev] = part[2 * q + 1]
        for c in (1, 0):
            for q in range(per):
                remote(inbox.at[c, q, pl.ds(1, n_lev - 1 - c)], part_send, part_recv.at[c, q]).wait_recv()
                total = inbox[c, q, 1]
                for e in range(2, n_lev):
                    total = total + inbox[c, q, e]
                partial[c, q] = total
                publish_first(c, q).start()
        for c in (1, 0):
            remote(inbox.at[c, :, 0], part_send, part_recv.at[c, per]).wait_recv()
            for q in range(per):
                total = inbox[c, q, 0] + partial[c, q]
                outgoing[c, q] = total
                if c == 1:
                    totals[side * per + q] = total
                for t in reversed(range(1, n_lev)):
                    pl.when(elsewhere(c, t))(lambda c=c, t=t, q=q: publish(c, t, q).start())

    @pl.when(hub)
    def _():
        relay(band).start()
        for c in range(2):
            for t in range(pairs):
                @pl.when(pair != t)
                def _(t=t, c=c):
                    came(2 * t + c)
                    relay(2 * t + c).start()
        came(band + 1)

    @pl.when(core == 1)
    def _():
        remote(whole.at[pl.ds(0, (n_band - 1) * blocks)], pass_sem, in_sem.at[0]).wait_recv()

    def pick(j, _):
        row = whole[pl.ds(source[j], 1), :]
        spread[pl.ds(pl.multiple_of(j * fields, fields), fields), :] = jnp.broadcast_to(row, (fields, lanes))
        return 0

    lax.fori_loop(0, blocks, pick, 0, unroll=32)

    def scale(i, _):
        span = pl.ds(pl.multiple_of(i * 64, 64), 64)
        local = jnp.tanh(spread[span, :])
        spread[span, :] = local

        def level(l, _):
            made[l, span, :] = (held[l, span, :].astype(jnp.float32) * (1.0 + taper[l] * local)).astype(made.dtype)
            return 0

        return lax.fori_loop(0, levels, level, 0, unroll=34)

    lax.fori_loop(0, rows // 64, scale, 0)

    pl.when(owner)(lambda: remote(totals.at[pl.ds(0, per)], part_send, total_recv).wait_recv())
    pl.when(jnp.logical_not(owner))(lambda: remote(totals, part_send, total_recv).wait_recv())
    for c in range(pieces):
        @pl.when(lev == 0)
        def _(c=c):
            totals[c] = part[2 * (c % per) + 1 - c // per] + totals[c]

        scaled = 1.0 / jnp.sqrt(totals[c, 2 * share:2 * share + 1, :])
        local = spread[pl.ds(c * share * fields, share, stride=fields), :] * scaled
        for k in range(2):
            sums[pl.ds(c * 2 * share + k, share, stride=2), :] = totals[c, k * share:(k + 1) * share, :] * local

    @pl.when(owner)
    def _():
        remote(part.at[pl.ds(0, per)], part_send, total_recv).wait_send()
        for c in range(2):
            remote(inbox.at[c, :, pl.ds(0, n_lev - c)], publish_send.at[c], total_recv).wait_send()

    pl.when(jnp.logical_not(owner))(lambda: remote(part, part_send, total_recv).wait_send())

    @pl.when(hub)
    def _():
        remote(whole.at[pl.ds(0, (pairs - 1) * blocks)], out_sem, total_recv).wait_send()
        remote(whole.at[pl.ds(0, (n_band - 1) * blocks)], pass_sem, total_recv).wait_send()

    pl.when(core == 1)(lambda: remote(whole.at[pl.ds(0, pairs * blocks)], out_sem, total_recv).wait_send())


def write(made, sums, out, column, out_sem, sum_sem):
    copies = (pltpu.make_async_copy(made, out, out_sem), pltpu.make_async_copy(sums, column, sum_sem))
    for copy in copies:
        copy.start()
    for copy in copies:
        copy.wait()


def body(n_band, n_lev, pattern, taper, thickness, block_source, tendencies):
    assert n_lev == 4 and n_band % 2 == 0
    fields, levels, columns = tendencies.shape
    blocks, lanes = pattern.shape
    rows = blocks * fields
    pieces = 4
    share, piece, pairs = blocks // pieces, rows // pieces, n_band // 2
    per = pieces // 2
    tend = tendencies.transpose(1, 0, 2).reshape(levels, fields, blocks, lanes)
    tend = tend.transpose(0, 2, 1, 3).reshape(levels, rows, lanes)
    hbm = pl.BlockSpec(memory_space=pltpu.HBM)
    vector = pl.BlockSpec(memory_space=pltpu.VMEM)
    f32, dma, flag = jnp.float32, pltpu.SemaphoreType.DMA, pltpu.SemaphoreType.REGULAR
    made, sums = pl.pallas_call(
        functools.partial(exchange, n_band, n_lev),
        name="exchange",
        out_shape=(pltpu.VMEM(tend.shape, tend.dtype), pltpu.VMEM((2 * blocks, lanes), f32)),
        in_specs=[hbm] * 5,
        out_specs=(vector, vector),
        scratch_shapes=[
            pltpu.VMEM(tend.shape, tend.dtype),
            pltpu.VMEM((rows, lanes), f32),
            pltpu.VMEM((n_band * blocks, lanes), f32),
            pltpu.VMEM((piece, lanes), f32),
            pltpu.VMEM((pieces, 2 * share + 1, lanes), f32),
            pltpu.VMEM((2, per, n_lev, 2 * share + 1, lanes), f32),
            pltpu.VMEM((pieces, 2 * share + 1, lanes), f32),
            pltpu.VMEM((2, per, 2 * share + 1, lanes), f32),
            pltpu.VMEM((2, per, 2 * share + 1, lanes), f32),
            pltpu.SMEM(block_source.shape, jnp.int32), pltpu.SMEM(taper.shape, f32), pltpu.SMEM(thickness.shape, f32),
            dma((3,)), dma, dma((pieces,)),
            flag, flag, flag, dma((n_band,)), dma((2, per + 1)), dma,
        ],
        compiler_params=pltpu.CompilerParams(collective_id=0, has_side_effects=True, vmem_limit_bytes=24 << 20),
    )(*(pltpu.with_memory_space_constraint(x, pltpu.MemorySpace.HBM)
        for x in (pattern, block_source, taper, thickness, tend)))
    in_vmem = lambda x: pltpu.with_memory_space_constraint(x, pltpu.MemorySpace.VMEM)
    out, column = pl.pallas_call(
        write,
        name="write",
        out_shape=(jax.ShapeDtypeStruct(tend.shape, tend.dtype), jax.ShapeDtypeStruct((2 * blocks, lanes), f32)),
        in_specs=[vector, vector],
        out_specs=(hbm, hbm),
        scratch_shapes=[dma, dma],
        compiler_params=pltpu.CompilerParams(vmem_limit_bytes=1 << 20),
    )(in_vmem(made), in_vmem(sums))
    out = out.reshape(levels, blocks, fields, lanes).transpose(2, 0, 1, 3).reshape(fields, levels, columns)
    return out, column.reshape(blocks, 2, lanes).transpose(1, 0, 2).reshape(2, columns)


def solution(mesh):
    in_specs = (P("band", None), P("lev"), P("lev"), P("band"), P(None, "lev", "band"))
    out_specs = (P(None, "lev", "band"), P(None, "band"))
    run = functools.partial(body, mesh.shape["band"], mesh.shape["lev"])
    return jax.shard_map(run, mesh=mesh, in_specs=in_specs, out_specs=out_specs, check_vma=False)
```

```python
import functools
import jax
import jax.numpy as jnp
from jax import lax
from jax.experimental import pallas as pl
from jax.experimental.pallas import tpu as pltpu
from jax.sharding import PartitionSpec as P

MESH = pl.DeviceIdType.MESH


def exchange(n_band, n_lev, pattern, source_hbm, taper_hbm, thickness_hbm, tend, made, sums,
             held, spread, whole, acc, part, inbox, totals, partial, outgoing, source, taper, thickness,
             small_sem, own_sem, load_sem, ready, mate_ready, lev_ready, in_sem, total_recv):
    band, lev = lax.axis_index("band"), lax.axis_index("lev")
    levels, rows, lanes = tend.shape
    blocks = pattern.shape[0]
    fields = rows // blocks
    pieces, half = totals.shape[0], n_lev // 2
    share, piece = blocks // pieces, rows // pieces
    pairs = n_band // 2
    per = pieces // 2
    side = lev // half
    near, far = half - 1 + side, half - side
    pair, core = band // 2, band % 2
    hub, keeper = core == 0, 2 * pair + 1
    owner = (core == 1) & (lev == near)
    out_sem, pass_sem, part_send, publish_send = own_sem, small_sem.at[0], small_sem.at[1], load_sem

    def signal(sem, **where):
        pl.semaphore_signal(sem, inc=1, device_id=where, device_id_type=MESH)

    def block_rows(who):
        return pl.ds(pl.multiple_of(who * blocks, blocks), blocks)

    own = pltpu.make_async_copy(pattern, whole.at[block_rows(band)], own_sem)
    own.start()
    small = [pltpu.make_async_copy(a, b, small_sem.at[i]) for i, (a, b) in enumerate(
        ((thickness_hbm, thickness), (taper_hbm, taper), (source_hbm, source)))]
    for copy in small:
        copy.start()

    def chunk_of(step):
        return (1 - side if step % 2 == 0 else side) * per + step // 2

    def load(step):
        span = pl.ds(pl.multiple_of(chunk_of(step) * piece, piece), piece)
        return pltpu.make_async_copy(tend.at[:, span, :], held.at[:, span, :], load_sem.at[step])

    barrier = pltpu.get_barrier_semaphore()
    for t in range(half - 1, half + 1):
        pl.when(lev < t)(lambda t=t: signal(barrier, band=keeper, lev=t))
    for t in range(half, n_lev):
        @pl.when(owner & (lev < t))
        def _(t=t):
            signal(barrier, band=2 * pair, lev=t)
            if t > half:
                signal(barrier, band=keeper, lev=t)
    for step in range(1):
        load(step).start()

    pl.when(hub)(lambda: signal(barrier, band=keeper))
    for t in range(1, pairs):
        @pl.when(pair < t)
        def _(t=t):
            signal(barrier, band=2 * t)
            pl.when(hub)(lambda: signal(barrier, band=2 * t + 1))
    from_band = jnp.where(hub, 2 * pair, pair + 1)
    from_lev = jnp.where(lev > half, 2, jnp.where(hub, lev // half, jnp.where(lev < half - 1, 0, 2 * lev)))
    expected = from_band + from_lev

    for step in range(1, pieces):
        load(step).start()

    def direct(t):
        mine = whole.at[block_rows(band)]
        return pltpu.make_async_remote_copy(mine, mine, out_sem, in_sem.at[band],
                                            device_id={"band": 2 * t}, device_id_type=MESH)

    def relay(origin):
        block = whole.at[block_rows(origin)]
        return pltpu.make_async_remote_copy(block, block, pass_sem, in_sem.at[0],
                                            device_id={"band": keeper}, device_id_type=MESH)

    def remote(ref, send, receive):
        return pltpu.make_async_remote_copy(ref, ref, send, receive,
                                            device_id={"lev": far}, device_id_type=MESH)

    def came(origin):
        remote(whole.at[block_rows(origin)], pass_sem, in_sem.at[origin]).wait_recv()

    def give(step):
        where = {"band": keeper, "lev": far if step % 2 == 0 else near}
        return pltpu.make_async_remote_copy(part.at[step], inbox.at[core, step // 2, lev], part_send,
                                            in_sem.at[1 + core * (per + 1) + jnp.where(lev == 0, per, step // 2)],
                                            device_id=where, device_id_type=MESH)

    def publish_first(c, q):
        return pltpu.make_async_remote_copy(partial.at[c, q], totals.at[side * per + q], publish_send.at[c], total_recv,
                                            device_id={"band": 2 * pair + c, "lev": 0}, device_id_type=MESH)

    def publish(c, t, q):
        return pltpu.make_async_remote_copy(outgoing.at[c, q], totals.at[side * per + q], publish_send.at[c], total_recv,
                                            device_id={"band": 2 * pair + c, "lev": t}, device_id_type=MESH)

    def elsewhere(c, t):
        return True if c == 0 else lev != t

    pl.when(expected > 0)(lambda: pl.semaphore_wait(barrier, expected))
    for t in range(half):
        @pl.when(owner & (lev > t))
        def _(t=t):
            signal(lev_ready, band=2 * pair, lev=t)
            signal(lev_ready, band=keeper, lev=t)
    pl.when(core == 1)(lambda: signal(mate_ready, band=2 * pair))
    for t in range(pairs - 1):
        @pl.when(hub & (pair > t))
        def _(t=t):
            signal(ready, band=2 * t)
            signal(ready, band=2 * t + 1)
    own.wait()
    for t in range(pairs):
        pl.when((pair > t) | ((core == 1) & (pair == t)))(lambda t=t: direct(t).start())

    for copy in small:
        copy.wait()
    squares = thickness[0] * thickness[0]
    for l in range(1, levels):
        squares += thickness[l] * thickness[l]
    pl.when(hub)(lambda: pl.semaphore_wait(mate_ready, 1))
    for step in range(pieces):
        load(step).wait()
        first = pl.multiple_of(chunk_of(step) * piece, piece)
        for r in range(0, piece, 64):
            def add(l, total):
                weight = thickness[l] * taper[l]
                return total + weight * held[l, pl.ds(first + r, 64), :].astype(jnp.float32)
            acc[pl.ds(r, 64), :] = lax.fori_loop(0, levels, add, jnp.zeros((64, lanes), jnp.float32), unroll=34)
        for k in range(2):
            part[step, k * share:(k + 1) * share, :] = acc[pl.ds(fields - 2 + k, share, stride=fields), :]
        part[step, 2 * share:, :] = jnp.full((1, lanes), squares, jnp.float32)
        if step == 0:
            pl.when(lev < half)(lambda: pl.semaphore_wait(lev_ready, jnp.where(lev < half - 1, 2, 1)))
        if step % 2 == 0:
            give(step).start()
        else:
            pl.when(jnp.logical_not(owner))(lambda step=step: give(step).start())
    pl.when(pair < pairs - 1)(lambda: pl.semaphore_wait(ready, pairs - 1 - pair))
    for t in range(1, pairs):
        pl.when(pair < t)(lambda t=t: direct(t).start())

    @pl.when(owner)
    def _():
        for q in range(per):
            inbox[1, q, lev] = part[2 * q + 1]
        for c, q in ((1, 0), (0, 0), (0, 1), (1, 1)):
            remote(inbox.at[c, q, pl.ds(1, n_lev - 1 - c)], part_send, in_sem.at[1 + c * (per + 1) + q]).wait_recv()
            total = inbox[c, q, 1]
            for e in range(2, n_lev):
                total = total + inbox[c, q, e]
            partial[c, q] = total
            publish_first(c, q).start()
        for c in (1, 0):
            remote(inbox.at[c, :, 0], part_send, in_sem.at[1 + c * (per + 1) + per]).wait_recv()
            for q in range(per):
                total = inbox[c, q, 0] + partial[c, q]
                outgoing[c, q] = total
                if c == 1:
                    totals[side * per + q] = total
                for t in reversed(range(1, n_lev)):
                    pl.when(elsewhere(c, t))(lambda c=c, t=t, q=q: publish(c, t, q).start())

    @pl.when(hub)
    def _():
        relay(band).start()
        for c in range(2):
            for t in range(pairs):
                @pl.when(pair != t)
                def _(t=t, c=c):
                    came(2 * t + c)
                    relay(2 * t + c).start()
        came(band + 1)

    @pl.when(core == 1)
    def _():
        remote(whole.at[pl.ds(0, (n_band - 1) * blocks)], pass_sem, in_sem.at[0]).wait_recv()

    def pick(j, _):
        row = whole[pl.ds(source[j], 1), :]
        spread[pl.ds(pl.multiple_of(j * fields, fields), fields), :] = jnp.broadcast_to(row, (fields, lanes))
        return 0

    lax.fori_loop(0, blocks, pick, 0, unroll=32)

    def scale(i, _):
        span = pl.ds(pl.multiple_of(i * 64, 64), 64)
        local = jnp.tanh(spread[span, :])
        spread[span, :] = local

        def level(l, _):
            made[l, span, :] = (held[l, span, :].astype(jnp.float32) * (1.0 + taper[l] * local)).astype(made.dtype)
            return 0

        return lax.fori_loop(0, levels, level, 0, unroll=34)

    lax.fori_loop(0, rows // 64, scale, 0)

    pl.when(owner)(lambda: remote(totals.at[pl.ds(0, per)], part_send, total_recv).wait_recv())
    pl.when(jnp.logical_not(owner))(lambda: remote(totals, part_send, total_recv).wait_recv())
    for c in range(pieces):
        @pl.when(lev == 0)
        def _(c=c):
            totals[c] = part[2 * (c % per) + 1 - c // per] + totals[c]

        scaled = 1.0 / jnp.sqrt(totals[c, 2 * share:2 * share + 1, :])
        local = spread[pl.ds(c * share * fields, share, stride=fields), :] * scaled
        for k in range(2):
            sums[pl.ds(c * 2 * share + k, share, stride=2), :] = totals[c, k * share:(k + 1) * share, :] * local

    @pl.when(owner)
    def _():
        remote(part.at[pl.ds(0, per)], part_send, total_recv).wait_send()
        for c in range(2):
            remote(inbox.at[c, :, pl.ds(0, n_lev - c)], publish_send.at[c], total_recv).wait_send()

    pl.when(jnp.logical_not(owner))(lambda: remote(part, part_send, total_recv).wait_send())

    @pl.when(hub)
    def _():
        remote(whole.at[pl.ds(0, (pairs - 1) * blocks)], out_sem, total_recv).wait_send()
        remote(whole.at[pl.ds(0, (n_band - 1) * blocks)], pass_sem, total_recv).wait_send()

    pl.when(core == 1)(lambda: remote(whole.at[pl.ds(0, pairs * blocks)], out_sem, total_recv).wait_send())


def write(made, sums, out, column, out_sem, sum_sem):
    copies = (pltpu.make_async_copy(made, out, out_sem), pltpu.make_async_copy(sums, column, sum_sem))
    for copy in copies:
        copy.start()
    for copy in copies:
        copy.wait()


def body(n_band, n_lev, pattern, taper, thickness, block_source, tendencies):
    assert n_lev == 4 and n_band % 2 == 0
    fields, levels, columns = tendencies.shape
    blocks, lanes = pattern.shape
    rows = blocks * fields
    pieces = 4
    share, piece, pairs = blocks // pieces, rows // pieces, n_band // 2
    per = pieces // 2
    tend = tendencies.transpose(1, 0, 2).reshape(levels, fields, blocks, lanes)
    tend = tend.transpose(0, 2, 1, 3).reshape(levels, rows, lanes)
    hbm = pl.BlockSpec(memory_space=pltpu.HBM)
    vector = pl.BlockSpec(memory_space=pltpu.VMEM)
    f32, dma, flag = jnp.float32, pltpu.SemaphoreType.DMA, pltpu.SemaphoreType.REGULAR
    made, sums = pl.pallas_call(
        functools.partial(exchange, n_band, n_lev),
        name="exchange",
        out_shape=(pltpu.VMEM(tend.shape, tend.dtype), pltpu.VMEM((2 * blocks, lanes), f32)),
        in_specs=[hbm] * 5,
        out_specs=(vector, vector),
        scratch_shapes=[
            pltpu.VMEM(tend.shape, tend.dtype),
            pltpu.VMEM((rows, lanes), f32),
            pltpu.VMEM((n_band * blocks, lanes), f32),
            pltpu.VMEM((piece, lanes), f32),
            pltpu.VMEM((pieces, 2 * share + 1, lanes), f32),
            pltpu.VMEM((2, per, n_lev, 2 * share + 1, lanes), f32),
            pltpu.VMEM((pieces, 2 * share + 1, lanes), f32),
            pltpu.VMEM((2, per, 2 * share + 1, lanes), f32),
            pltpu.VMEM((2, per, 2 * share + 1, lanes), f32),
            pltpu.SMEM(block_source.shape, jnp.int32), pltpu.SMEM(taper.shape, f32), pltpu.SMEM(thickness.shape, f32),
            dma((3,)), dma, dma((pieces,)),
            flag, flag, flag, dma((max(n_band, 2 * per + 3),)), dma,
        ],
        compiler_params=pltpu.CompilerParams(collective_id=0, has_side_effects=True, vmem_limit_bytes=24 << 20),
    )(*(pltpu.with_memory_space_constraint(x, pltpu.MemorySpace.HBM)
        for x in (pattern, block_source, taper, thickness, tend)))
    in_vmem = lambda x: pltpu.with_memory_space_constraint(x, pltpu.MemorySpace.VMEM)
    out, column = pl.pallas_call(
        write,
        name="write",
        out_shape=(jax.ShapeDtypeStruct(tend.shape, tend.dtype), jax.ShapeDtypeStruct((2 * blocks, lanes), f32)),
        in_specs=[vector, vector],
        out_specs=(hbm, hbm),
        scratch_shapes=[dma, dma],
        compiler_params=pltpu.CompilerParams(vmem_limit_bytes=1 << 20),
    )(in_vmem(made), in_vmem(sums))
    out = out.reshape(levels, blocks, fields, lanes).transpose(2, 0, 1, 3).reshape(fields, levels, columns)
    return out, column.reshape(blocks, 2, lanes).transpose(1, 0, 2).reshape(2, columns)


def solution(mesh):
    in_specs = (P("band", None), P("lev"), P("lev"), P("band"), P(None, "lev", "band"))
    out_specs = (P(None, "lev", "band"), P(None, "band"))
    run = functools.partial(body, mesh.shape["band"], mesh.shape["lev"])
    return jax.shard_map(run, mesh=mesh, in_specs=in_specs, out_specs=out_specs, check_vma=False)
```
